32 devices in a mesh: dp: 16 (over z, x, core), owner: 2 (over y).
Axes of the slice: x: 2, y: 2, z: 4, core: 2. Of those that a mesh axis runs over, the one named last changes fastest.
Arguments:
- edge_in: bfloat16 [2, 8192, 512], P(None, ('dp', 'owner')), may hold values from -256 to 256
- edge_grad: bfloat16 [2, 8192, 512], P(None, ('dp', 'owner')), may hold values from -1.1953125 to 1.1953125
- row_mask: int32 [2, 8192], P(None, ('dp', 'owner')), may hold values 0 or 1
- layer_at: int32 [2], replicated, may hold values from 0 to 1, each once
Outputs:
- update: bfloat16 [2, 512, 512], P('owner')
The draws below stay inside these ranges and needn't reach their ends.
Inputs may be any that keep to these rules, and one draw needn't show every extreme that they name: `layer_at`: every layer number appears once.
All inputs are finite; a program needn't handle non-finite values. No bound on the sum of `row_mask` on one device may be relied on, other than what follows from the above.
Results may differ from the reference program's by a relative error of at most 0.0085.
Values may be sent and summed in bfloat16 or wider, within the bound.
A program may use at most 64 MiB of HBM per device.

```python
import math
import jax
import jax.numpy as jnp
from jax import lax

D = 512
LAYERS = 2
ROWS_DEV = 256
ROWS_ALL = 8192
ITERS = 4


def draw_edge_in(key, part):
    base = jax.random.fold_in(key, 11)
    key_a, key_b = jax.random.split(base, 2)
    normal_part = jnp.clip(jax.random.normal(key_a, (LAYERS, ROWS_ALL, D), jnp.float32), -6.0, 6.0)
    unit = jax.random.uniform(key_b, (LAYERS, ROWS_ALL, 1), jnp.float32)
    scale = jnp.exp(unit * jnp.log(10.0))
    values = scale * normal_part
    return jnp.clip(values, -256.0, 256.0).astype(jnp.bfloat16)


def plant(entries, stream_key, least, largest):
    extent = entries.shape
    index_at = [jax.random.randint(jax.random.fold_in(stream_key, axis), (), 0, extent[axis]) for axis in range(len(extent))]
    entries = entries.at[tuple(index_at)].set(least)
    longest = extent.index(max(extent))
    index_at[longest] = (index_at[longest] + 1) % extent[longest]
    return entries.at[tuple(index_at)].set(largest)


def steps_of(own_key, shape, cuts, least, largest):
    def one(dim, parts):
        steps = jax.random.uniform(jax.random.fold_in(jax.random.fold_in(own_key, 6), dim), (parts,), jnp.float32, least / len(cuts), largest / len(cuts))
        return jnp.repeat(jnp.exp(steps), shape[dim] // parts).reshape((-1,) + (1,) * (len(shape) - dim - 1))

    gain = one(*cuts[0])
    for cut in cuts[1:]:
        gain = gain * one(*cut)
    return gain


def normal_values(stream_key, shape, deviation, bound, cuts=(), held_as=jnp.bfloat16):
    values = deviation * jax.random.normal(stream_key, shape, jnp.float32)
    if cuts:
        values = values * steps_of(stream_key, shape, cuts, -0.22, 0.18)
    return jnp.clip(values, -bound, bound).astype(held_as)


def setup_inputs(seed: int = 0) -> dict:
    key_list = jax.random.split(jax.random.key(seed), 5)
    return {
        "edge_in": draw_edge_in(jax.random.fold_in(key_list[4], 71), 0),
        "edge_grad": normal_values(key_list[1], (LAYERS, ROWS_ALL, D), 0.2, 1.1953125, ((1, 32),)),
        "row_mask": plant((jax.random.randint(key_list[2], (LAYERS, ROWS_ALL), 0, 2) < 1).astype(jnp.int32), jax.random.fold_in(key_list[2], 1), 0, 1),
        "layer_at": jax.random.permutation(key_list[3], LAYERS).astype(jnp.int32),
    }


def newton(factor):
    eye = jnp.eye(D, dtype=jnp.float32)
    damped = factor + jnp.trace(factor) * (0.05 / D) * eye
    size_sq = jnp.sqrt(jnp.sum(damped * damped) + 1e-06)
    approx = eye / size_sq
    for step in range(ITERS):
        inner = jnp.matmul(damped, approx, precision=lax.Precision.HIGHEST)
        approx = 2.0 * approx - jnp.matmul(approx, inner, precision=lax.Precision.HIGHEST)
    return approx

def precondition(packed):
    factor_in, factor_out, grad = packed
    inv_in = newton(factor_in)
    inv_out = newton(factor_out)
    left = jnp.matmul(inv_in, grad, precision=lax.Precision.HIGHEST)
    return jnp.matmul(left, inv_out, precision=lax.Precision.HIGHEST)

def reference(edge_in, edge_grad, row_mask, layer_at):
    scale_factor = 1.0 / ROWS_ALL
    scale_grad = 1.0 / math.sqrt(ROWS_ALL)

    def add_block(index, carry):
        total_in, total_out, total_grad = carry
        start = index * ROWS_DEV
        inputs = lax.dynamic_slice_in_dim(edge_in, start, ROWS_DEV, 1).astype(jnp.float32)
        grads = lax.dynamic_slice_in_dim(edge_grad, start, ROWS_DEV, 1).astype(jnp.float32)
        weights = lax.dynamic_slice_in_dim(row_mask, start, ROWS_DEV, 1).astype(jnp.float32)[..., None]
        kept_in = inputs * weights
        kept_grad = grads * weights
        term_in = (jnp.einsum('lrd,lre->lde', kept_in, kept_in) * scale_factor).astype(jnp.bfloat16)
        term_out = (jnp.einsum('lrd,lre->lde', kept_grad, kept_grad) * scale_factor).astype(jnp.bfloat16)
        term_grad = (jnp.einsum('lrd,lre->lde', inputs, grads) * scale_grad).astype(jnp.bfloat16)
        term_in, term_out, term_grad = lax.optimization_barrier((term_in, term_out, term_grad))
        return (total_in + term_in.astype(jnp.float32), total_out + term_out.astype(jnp.float32), total_grad + term_grad.astype(jnp.float32))
    zeros = jnp.zeros((LAYERS, D, D), jnp.float32)
    factor_in, factor_out, grad = lax.fori_loop(0, ROWS_ALL // ROWS_DEV, add_block, (zeros, zeros, zeros))
    picked = (jnp.take(factor_in, layer_at, axis=0), jnp.take(factor_out, layer_at, axis=0), jnp.take(grad, layer_at, axis=0))
    update = lax.map(precondition, picked)
    return update.astype(jnp.bfloat16)
```

```python
import functools
import math

import jax
import jax.numpy as jnp
from jax import lax
from jax.experimental import pallas as pl
from jax.experimental.pallas import tpu as pltpu
from jax.sharding import PartitionSpec as P

MESH = pl.DeviceIdType.MESH
F32 = jnp.float32
BF16 = jnp.bfloat16


def mm(left, right):
    return jnp.dot(left, right, preferred_element_type=F32)


def mm_rows(left, right):
    return lax.dot_general(left, right, (((0,), (0,)), ((), ())), preferred_element_type=F32)


def kernel(
    owners, chips, slots, rows, width, rows_all,
    edge_in, edge_grad, mask, layer_at, out,
    picked, picked_mask, rows_got, mask_got,
    give, got, split, split_got, total, halves, inverse,
    row_send, row_recv, mask_send, mask_recv, core_send, core_recv,
    split_send, split_recv, total_send, total_recv,
):
    dp = lax.axis_index("dp")
    me = lax.axis_index("owner")
    chip = dp // 2
    core = lax.rem(dp, 2)
    other = 1 - core
    half = width // 2
    part = (width + half) // chips

    barrier = pltpu.get_barrier_semaphore()

    def owner_at(k):
        return {"dp": dp, "owner": lax.rem(me + k, owners)}

    def chip_at(k):
        return {"dp": lax.rem(chip + k, chips) * 2 + core, "owner": me}

    partner = {"dp": chip * 2 + other, "owner": me}
    peers = [owner_at(k) for k in range(1, owners)]
    peers += [chip_at(k) for k in range(1, chips)]
    peers += [partner]
    for peer in peers:
        pl.semaphore_signal(barrier, inc=1, device_id=peer, device_id_type=MESH)

    for q in range(owners):
        for s in range(slots):
            layer = layer_at[q * slots + s]
            picked[q, 0, s] = edge_in[layer]
            picked[q, 1, s] = edge_grad[layer]
            line = mask[pl.ds(layer, 1), :].astype(F32)
            picked_mask[q, s] = jnp.broadcast_to(line, (8, rows))
    pl.semaphore_wait(barrier, len(peers))

    def copy(src, dst, send, recv, device):
        made = pltpu.make_async_remote_copy(
            src_ref=src, dst_ref=dst, send_sem=send, recv_sem=recv,
            device_id=device, device_id_type=MESH,
        )
        made.start()
        return made

    started = []
    row_copies = []
    for k in range(1, owners):
        to = lax.rem(me + k, owners)
        row_copies.append(copy(picked_mask.at[to], mask_got.at[k - 1], mask_send.at[k - 1], mask_recv.at[k - 1], owner_at(k)))
    for t in range(2):
        for k in range(1, owners):
            to = lax.rem(me + k, owners)
            row_copies.append(copy(picked.at[to, t], rows_got.at[k - 1, t], row_send.at[k - 1, t], row_recv.at[k - 1, t], owner_at(k)))
    for c in row_copies:
        c.wait_recv()
    started += row_copies

    def kept(values, line):
        column = jnp.broadcast_to(line[0:1, :], (128, rows)).T
        column = jnp.concatenate([column] * (width // 128), axis=1)
        return (values.astype(F32) * column).astype(BF16)

    def terms(c, s):
        factor = None
        cross = None
        for k in range(owners):
            if k == 0:
                block, line = picked.at[me], picked_mask[me, s]
            else:
                block, line = rows_got.at[k - 1], mask_got[k - 1, s]
            values = kept(block[c, s], line)
            left = block[0, s, :, pl.ds(pl.multiple_of(c * half, half), half)]
            a = mm_rows(values, values)
            b = mm_rows(left, block[1, s])
            factor = a if factor is None else factor + a
            cross = b if cross is None else cross + b
        return factor * (1.0 / rows_all), cross * (1.0 / math.sqrt(rows_all))

    core_copies = []
    for s in range(slots):
        factor, cross = terms(other, s)
        give[s, :width] = factor.astype(BF16)
        give[s, width:] = cross.astype(BF16)
        core_copies.append(copy(give.at[s], got.at[s], core_send.at[s], core_recv.at[s], partner))
    started += core_copies

    for s in range(slots):
        factor, cross = terms(core, s)
        core_copies[s].wait_recv()
        both = jnp.concatenate([factor, cross], axis=0) + got[s].astype(F32)
        split[:, s] = both.astype(BF16).reshape(chips, part, width)

    split_copies = []
    for k in range(1, chips):
        to = lax.rem(chip + k, chips)
        split_copies.append(copy(split.at[to], split_got.at[k - 1], split_send.at[k - 1], split_recv.at[k - 1], chip_at(k)))
    started += split_copies
    summed = split[chip].astype(F32)
    for k in range(1, chips):
        split_copies[k - 1].wait_recv()
        summed += split_got[k - 1].astype(F32)
    total[chip] = summed.astype(BF16)

    total_copies = []
    for k in range(1, chips):
        total_copies.append(copy(total.at[chip], total.at[chip], total_send.at[k - 1], total_recv.at[k - 1], chip_at(k)))
    started += total_copies
    for c in total_copies:
        c.wait_recv()

    at_row = lax.broadcasted_iota(jnp.int32, (width, width), 0)
    at_column = lax.broadcasted_iota(jnp.int32, (width, width), 1)
    eye = (at_row == at_column).astype(F32)
    half_copies = []
    inverse_copies = []
    for s in range(slots):
        whole = total[:, s].reshape(width + half, width)
        halves[core, s] = whole[width:]
        half_copies.append(copy(halves.at[core, s], halves.at[core, s], core_send.at[slots + s], core_recv.at[slots + s], partner))
    for s in range(slots):
        whole = total[:, s].reshape(width + half, width)
        factor = whole[:width].astype(F32)
        damped = factor + (jnp.sum(factor * eye) * (0.05 / width)) * eye
        scale = lax.rsqrt(jnp.sum(damped * damped) + 1e-06)
        near = damped * scale
        approx = 2.0 * eye - near
        near_low = near.astype(BF16)
        near = 2.0 * near - mm(near_low, near_low)
        for step in range(3):
            near_low = near.astype(BF16)
            approx = 2.0 * approx - mm(approx.astype(BF16), near_low)
            if step < 2:
                near = 2.0 * near - mm(near_low, near_low)
        inverse[core, s] = (approx * scale).astype(BF16)
        inverse_copies.append(copy(inverse.at[core, s], inverse.at[core, s], core_send.at[2 * slots + s], core_recv.at[2 * slots + s], partner))
    started += half_copies + inverse_copies
    for s in range(slots):
        half_copies[s].wait_recv()
        inverse_copies[s].wait_recv()
        grad = halves[:, s].reshape(width, width)
        left = mm(inverse[0, s], grad)
        out[s] = mm(left.astype(BF16), inverse[1, s]).astype(BF16)
    for c in started:
        c.wait_send()


def solution(mesh):
    owners = mesh.shape["owner"]
    chips = mesh.shape["dp"] // 2

    def local(edge_in, edge_grad, row_mask, layer_at):
        layers, rows, width = edge_in.shape
        slots = layers // owners
        rows_all = rows * mesh.shape["dp"] * owners
        high = width + width // 2
        part = high // chips
        others = max(owners - 1, 1)
        vmem = pl.BlockSpec(memory_space=pltpu.VMEM)
        dma = pltpu.SemaphoreType.DMA
        return pl.pallas_call(
            functools.partial(kernel, owners, chips, slots, rows, width, rows_all),
            out_shape=jax.ShapeDtypeStruct((slots, width, width), BF16),
            in_specs=[vmem, vmem, vmem, pl.BlockSpec(memory_space=pltpu.SMEM)],
            out_specs=vmem,
            scratch_shapes=[
                pltpu.VMEM((owners, 2, slots, rows, width), BF16),
                pltpu.VMEM((owners, slots, 8, rows), F32),
                pltpu.VMEM((others, 2, slots, rows, width), BF16),
                pltpu.VMEM((others, slots, 8, rows), F32),
                pltpu.VMEM((slots, high, width), BF16),
                pltpu.VMEM((slots, high, width), BF16),
                pltpu.VMEM((chips, slots, part, width), BF16),
                pltpu.VMEM((chips - 1, slots, part, width), BF16),
                pltpu.VMEM((chips, slots, part, width), BF16),
                pltpu.VMEM((2, slots, width // 2, width), BF16),
                pltpu.VMEM((2, slots, width, width), BF16),
                dma((others, 2)), dma((others, 2)),
                dma((others,)), dma((others,)),
                dma((3 * slots,)), dma((3 * slots,)),
                dma((chips - 1,)), dma((chips - 1,)),
                dma((chips - 1,)), dma((chips - 1,)),
            ],
            compiler_params=pltpu.CompilerParams(
                collective_id=0, has_side_effects=True, vmem_limit_bytes=60 * 1024 * 1024,
            ),
        )(edge_in, edge_grad, row_mask, layer_at)

    in_specs = (
        P(None, ("dp", "owner"), None),
        P(None, ("dp", "owner"), None),
        P(None, ("dp", "owner")),
        P(),
    )
    return jax.shard_map(local, mesh=mesh, in_specs=in_specs, out_specs=P("owner", None, None), check_vma=False)
```

```python
import functools
import math

import jax
import jax.numpy as jnp
from jax import lax
from jax.experimental import pallas as pl
from jax.experimental.pallas import tpu as pltpu
from jax.sharding import PartitionSpec as P

MESH = pl.DeviceIdType.MESH
F32 = jnp.float32
BF16 = jnp.bfloat16
TILE = 128


def mm(left, right):
    return jnp.dot(left, right, preferred_element_type=F32)


def mm_rows(left, right):
    return lax.dot_general(left, right, (((0,), (0,)), ((), ())), preferred_element_type=F32)


def kernel(
    owners, chips, slots, rows, width, rows_all,
    edge_in, edge_grad, mask, layer_at, out,
    picked, picked_mask, rows_got, mask_got,
    give, got, split, pair_got, passing, line_got, total, full, halves, inverse,
    row_send, row_recv, mask_send, mask_recv, core_send, core_recv,
    pair_send, pair_recv, line_send, line_recv,
    spread_send, spread_recv, across_send, across_recv,
):
    dp = lax.axis_index("dp")
    me = lax.axis_index("owner")
    chip = dp // 2
    core = lax.rem(dp, 2)
    other = 1 - core
    half = width // 2
    part = TILE // chips
    tiles = width // TILE
    lines = chips // 2
    line = chip // 2
    side = lax.rem(chip, 2)

    barrier = pltpu.get_barrier_semaphore()

    def owner_at(k):
        return {"dp": dp, "owner": lax.rem(me + k, owners)}

    def line_at(k):
        return {"dp": (lax.rem(line + k, lines) * 2 + side) * 2 + core, "owner": me}

    pair = {"dp": (line * 2 + 1 - side) * 2 + core, "owner": me}

    partner = {"dp": chip * 2 + other, "owner": me}
    peers = [owner_at(k) for k in range(1, owners)]
    peers += [line_at(k) for k in range(1, lines)]
    peers += [pair, partner]
    for peer in peers:
        pl.semaphore_signal(barrier, inc=1, device_id=peer, device_id_type=MESH)

    for q in range(owners):
        for s in range(slots):
            layer = layer_at[q * slots + s]
            picked[q, 0, s] = edge_in[layer]
            picked[q, 1, s] = edge_grad[layer]
            mask_row = mask[pl.ds(layer, 1), :].astype(F32)
            picked_mask[q, s] = jnp.broadcast_to(mask_row, (8, rows))
    pl.semaphore_wait(barrier, len(peers))

    def copy(src, dst, send, recv, device):
        made = pltpu.make_async_remote_copy(
            src_ref=src, dst_ref=dst, send_sem=send, recv_sem=recv,
            device_id=device, device_id_type=MESH,
        )
        made.start()
        return made

    started = []
    row_copies = []
    for k in range(1, owners):
        to = lax.rem(me + k, owners)
        row_copies.append(copy(picked_mask.at[to], mask_got.at[k - 1], mask_send.at[k - 1], mask_recv.at[k - 1], owner_at(k)))
    for t in range(2):
        for k in range(1, owners):
            to = lax.rem(me + k, owners)
            row_copies.append(copy(picked.at[to, t], rows_got.at[k - 1, t], row_send.at[k - 1, t], row_recv.at[k - 1, t], owner_at(k)))
    for c in row_copies:
        c.wait_recv()
    started += row_copies

    def kept(values, line):
        column = jnp.broadcast_to(line[0:1, :], (128, rows)).T
        column = jnp.concatenate([column] * (width // 128), axis=1)
        return (values.astype(F32) * column).astype(BF16)

    def terms(c, s):
        sums = {}
        for k in range(owners):
            if k == 0:
                block, line_mask = picked.at[me], picked_mask[me, s]
            else:
                block, line_mask = rows_got.at[k - 1], mask_got[k - 1, s]
            values = kept(block[c, s], line_mask)
            left = block[0, s, :, pl.ds(pl.multiple_of(c * half, half), half)]
            made = [mm_rows(values[:, TILE * i:TILE * (i + 1)], values[:, TILE * i:]) for i in range(tiles)]
            made.append(mm_rows(left, block[1, s]))
            for i, value in enumerate(made):
                sums[i] = sums[i] + value if k else value
        return sums

    def pack(ref, s, sums):
        at = 0
        for i in range(tiles):
            strip = sums[i] * (1.0 / rows_all)
            for j in range(tiles - i):
                tile = strip[:, TILE * j:TILE * (j + 1)].reshape(chips, part, TILE)
                ref[s, :, at] = tile.astype(BF16)
                at += 1
        cross = sums[tiles] * (1.0 / math.sqrt(rows_all))
        for i in range(tiles // 2):
            for j in range(tiles):
                tile = cross[TILE * i:TILE * (i + 1), TILE * j:TILE * (j + 1)].reshape(chips, part, TILE)
                ref[s, :, at] = tile.astype(BF16)
                at += 1

    def tile_of(s, at):
        return total[:, s, at].astype(F32).reshape(TILE, TILE)

    core_copies = []
    for s in range(slots):
        pack(give, s, terms(other, s))
        core_copies.append(copy(give.at[s], got.at[s], core_send.at[s], core_recv.at[s], partner))
    started += core_copies

    for s in range(slots):
        pack(split, s, terms(core, s))
        core_copies[s].wait_recv()
        split[s] = (split[s].astype(F32) + got[s].astype(F32)).astype(BF16)

    order = list(range(1, lines)) + [0]
    pair_copies = {}
    for k in order:
        far = lax.rem(line + k, lines) * 2 + 1 - side
        pair_copies[k] = copy(split.at[:, far], pair_got.at[k], pair_send.at[k], pair_recv.at[k], pair)
    line_copies = {}
    for k in order:
        near = lax.rem(line + k, lines) * 2 + side
        pair_copies[k].wait_recv()
        summed = split[:, near].astype(F32) + pair_got[k].astype(F32)
        if k:
            passing[k - 1] = summed.astype(BF16)
            line_copies[k] = copy(passing.at[k - 1], line_got.at[k - 1], line_send.at[k - 1], line_recv.at[k - 1], line_at(k))
    for k in range(1, lines):
        line_copies[k].wait_recv()
        summed += line_got[k - 1].astype(F32)
    total[chip] = summed.astype(BF16)
    started += list(pair_copies.values()) + list(line_copies.values())

    spread = {}
    for k in range(1, lines):
        spread[k] = copy(total.at[chip], total.at[chip], spread_send.at[k - 1], spread_recv.at[k - 1], line_at(k))
    across = [copy(total.at[chip], total.at[chip], across_send.at[0], across_recv.at[0], pair)]
    for k in range(1, lines):
        spread[k].wait_recv()
        origin = lax.rem(line - k + lines, lines) * 2 + side
        across.append(copy(total.at[origin], total.at[origin], across_send.at[k], across_recv.at[k], pair))
    for c in across:
        c.wait_recv()
    started += list(spread.values()) + across

    at_row = lax.broadcasted_iota(jnp.int32, (width, width), 0)
    at_column = lax.broadcasted_iota(jnp.int32, (width, width), 1)
    eye = (at_row == at_column).astype(F32)
    half_copies = []
    inverse_copies = []
    for s in range(slots):
        at = tiles * (tiles + 1) // 2
        for i in range(tiles // 2):
            for j in range(tiles):
                halves[core, s, TILE * i:TILE * (i + 1), TILE * j:TILE * (j + 1)] = tile_of(s, at).astype(BF16)
                at += 1
        half_copies.append(copy(halves.at[core, s], halves.at[core, s], core_send.at[slots + s], core_recv.at[slots + s], partner))
    for s in range(slots):
        at = 0
        for i in range(tiles):
            for j in range(i, tiles):
                tile = tile_of(s, at)
                full[TILE * i:TILE * (i + 1), TILE * j:TILE * (j + 1)] = tile
                if j > i:
                    full[TILE * j:TILE * (j + 1), TILE * i:TILE * (i + 1)] = tile.T
                at += 1
        factor = full[...]
        damped = factor + (jnp.sum(factor * eye) * (0.05 / width)) * eye
        scale = lax.rsqrt(jnp.sum(damped * damped) + 1e-06)
        near = damped * scale
        approx = 2.0 * eye - near
        near_low = near.astype(BF16)
        near = 2.0 * near - mm(near_low, near_low)
        for step in range(3):
            near_low = near.astype(BF16)
            approx = 2.0 * approx - mm(approx.astype(BF16), near_low)
            if step < 2:
                near = 2.0 * near - mm(near_low, near_low)
        inverse[core, s] = (approx * scale).astype(BF16)
        inverse_copies.append(copy(inverse.at[core, s], inverse.at[core, s], core_send.at[2 * slots + s], core_recv.at[2 * slots + s], partner))
    started += half_copies + inverse_copies
    for s in range(slots):
        half_copies[s].wait_recv()
        inverse_copies[s].wait_recv()
        grad = halves[:, s].reshape(width, width)
        left = mm(inverse[0, s], grad)
        out[s] = mm(left.astype(BF16), inverse[1, s]).astype(BF16)
    for c in started:
        c.wait_send()


def solution(mesh):
    owners = mesh.shape["owner"]
    chips = mesh.shape["dp"] // 2

    def local(edge_in, edge_grad, row_mask, layer_at):
        layers, rows, width = edge_in.shape
        slots = layers // owners
        rows_all = rows * mesh.shape["dp"] * owners
        tiles = width // TILE
        count = tiles * (tiles + 1) // 2 + tiles * tiles // 2
        part = TILE // chips
        lines = chips // 2
        others = max(owners - 1, 1)
        vmem = pl.BlockSpec(memory_space=pltpu.VMEM)
        dma = pltpu.SemaphoreType.DMA
        return pl.pallas_call(
            functools.partial(kernel, owners, chips, slots, rows, width, rows_all),
            out_shape=jax.ShapeDtypeStruct((slots, width, width), BF16),
            in_specs=[vmem, vmem, vmem, pl.BlockSpec(memory_space=pltpu.SMEM)],
            out_specs=vmem,
            scratch_shapes=[
                pltpu.VMEM((owners, 2, slots, rows, width), BF16),
                pltpu.VMEM((owners, slots, 8, rows), F32),
                pltpu.VMEM((others, 2, slots, rows, width), BF16),
                pltpu.VMEM((others, slots, 8, rows), F32),
                pltpu.VMEM((slots, chips, count, part, TILE), BF16),
                pltpu.VMEM((slots, chips, count, part, TILE), BF16),
                pltpu.VMEM((slots, chips, count, part, TILE), BF16),
                pltpu.VMEM((lines, slots, count, part, TILE), BF16),
                pltpu.VMEM((lines - 1, slots, count, part, TILE), BF16),
                pltpu.VMEM((lines - 1, slots, count, part, TILE), BF16),
                pltpu.VMEM((chips, slots, count, part, TILE), BF16),
                pltpu.VMEM((width, width), F32),
                pltpu.VMEM((2, slots, width // 2, width), BF16),
                pltpu.VMEM((2, slots, width, width), BF16),
                dma((others, 2)), dma((others, 2)),
                dma((others,)), dma((others,)),
                dma((3 * slots,)), dma((3 * slots,)),
                dma((lines,)), dma((lines,)),
                dma((lines - 1,)), dma((lines - 1,)),
                dma((lines - 1,)), dma((lines - 1,)),
                dma((lines,)), dma((lines,)),
            ],
            compiler_params=pltpu.CompilerParams(
                collective_id=0, has_side_effects=True, vmem_limit_bytes=60 * 1024 * 1024,
            ),
        )(edge_in, edge_grad, row_mask, layer_at)

    in_specs = (
        P(None, ("dp", "owner"), None),
        P(None, ("dp", "owner"), None),
        P(None, ("dp", "owner")),
        P(),
    )
    return jax.shard_map(local, mesh=mesh, in_specs=in_specs, out_specs=P("owner", None, None), check_vma=False)
```

```python
import functools
import math

import jax
import jax.numpy as jnp
from jax import lax
from jax.experimental import pallas as pl
from jax.experimental.pallas import tpu as pltpu
from jax.sharding import PartitionSpec as P

MESH = pl.DeviceIdType.MESH
F32 = jnp.float32
BF16 = jnp.bfloat16
TILE = 128


def mm(left, right):
    return jnp.dot(left, right, preferred_element_type=F32)


def mm_rows(left, right):
    return lax.dot_general(left, right, (((0,), (0,)), ((), ())), preferred_element_type=F32)


def kernel(
    owners, chips, slots, rows, width, rows_all,
    edge_in, edge_grad, mask, layer_at, out,
    give, got, split, pair_got, crossing, owner_got, passing, line_got, total, full, halves, inverse,
    core_send, core_recv, pair_send, pair_recv, owner_send, owner_recv,
    line_send, line_recv, last_send, last_recv,
    spread_send, spread_recv, across_send, across_recv,
):
    dp = lax.axis_index("dp")
    me = lax.axis_index("owner")
    chip = dp // 2
    core = lax.rem(dp, 2)
    other = 1 - core
    half = width // 2
    part = TILE // chips
    tiles = width // TILE
    lines = chips // 2
    line = chip // 2
    side = lax.rem(chip, 2)

    barrier = pltpu.get_barrier_semaphore()

    def owner_at(k):
        return {"dp": dp, "owner": lax.rem(me + k, owners)}

    def line_at(k):
        return {"dp": (lax.rem(line + k, lines) * 2 + side) * 2 + core, "owner": me}

    pair = {"dp": (line * 2 + 1 - side) * 2 + core, "owner": me}

    partner = {"dp": chip * 2 + other, "owner": me}
    peers = [owner_at(k) for k in range(1, owners)]
    peers += [line_at(k) for k in range(1, lines)]
    peers += [pair, partner]
    for peer in peers:
        pl.semaphore_signal(barrier, inc=1, device_id=peer, device_id_type=MESH)

    def copy(src, dst, send, recv, device):
        made = pltpu.make_async_remote_copy(
            src_ref=src, dst_ref=dst, send_sem=send, recv_sem=recv,
            device_id=device, device_id_type=MESH,
        )
        made.start()
        return made

    started = []

    def terms(c, q, s):
        layer = layer_at[q * slots + s]
        inputs, grads = edge_in[layer], edge_grad[layer]
        column = jnp.broadcast_to(mask[pl.ds(layer, 1), :].astype(F32), (TILE, rows)).T
        column = jnp.concatenate([column] * tiles, axis=1)
        first = c == 0
        values = (jnp.where(first, inputs, grads).astype(F32) * column).astype(BF16)
        left = jnp.where(first, inputs[:, :half], inputs[:, half:])
        made = [mm_rows(values[:, TILE * i:TILE * (i + 1)], values[:, TILE * i:]) for i in range(tiles)]
        made.append(mm_rows(left, grads))
        return made

    def pack(ref, sums):
        at = 0
        for i in range(tiles):
            strip = sums[i] * (1.0 / rows_all)
            for j in range(tiles - i):
                tile = strip[:, TILE * j:TILE * (j + 1)].reshape(chips, part, TILE)
                ref[:, at] = tile.astype(BF16)
                at += 1
        cross = sums[tiles] * (1.0 / math.sqrt(rows_all))
        for i in range(tiles // 2):
            for j in range(tiles):
                tile = cross[TILE * i:TILE * (i + 1), TILE * j:TILE * (j + 1)].reshape(chips, part, TILE)
                ref[:, at] = tile.astype(BF16)
                at += 1

    def tile_of(s, at):
        return total[:, s, at].astype(F32).reshape(TILE, TILE)

    order = list(range(1, lines)) + [0]
    pair_copies = {}
    for o in list(range(1, owners)) + [0]:
        q = lax.rem(me + o, owners)
        core_copies = []
        for s in range(slots):
            pack(give.at[o, s], terms(other, q, s))
            if not started and not core_copies:
                pl.semaphore_wait(barrier, len(peers))
            core_copies.append(copy(give.at[o, s], got.at[o, s], core_send.at[o, s], core_recv.at[o, s], partner))
        for s in range(slots):
            pack(split.at[o, s], terms(core, q, s))
            core_copies[s].wait_recv()
            split[o, s] = (split[o, s].astype(F32) + got[o, s].astype(F32)).astype(BF16)
        started += core_copies
        for k in order:
            far = lax.rem(line + k, lines) * 2 + 1 - side
            pair_copies[o, k] = copy(split.at[o, :, far], pair_got.at[o, k], pair_send.at[o, k], pair_recv.at[o, k], pair)

    owner_copies = {}
    for o in range(1, owners):
        for k in order:
            near = lax.rem(line + k, lines) * 2 + side
            pair_copies[o, k].wait_recv()
            crossing[o - 1, k] = (split[o, :, near].astype(F32) + pair_got[o, k].astype(F32)).astype(BF16)
            owner_copies[o, k] = copy(crossing.at[o - 1, k], owner_got.at[o - 1, k], owner_send.at[o - 1, k], owner_recv.at[o - 1, k], owner_at(o))
    line_copies = {}
    for k in order:
        near = lax.rem(line + k, lines) * 2 + side
        pair_copies[0, k].wait_recv()
        summed = split[0, :, near].astype(F32) + pair_got[0, k].astype(F32)
        for o in range(1, owners):
            owner_copies[o, k].wait_recv()
            summed += owner_got[o - 1, k].astype(F32)
        if k:
            passing[k - 1] = summed.astype(BF16)
            line_copies[k] = copy(passing.at[k - 1], line_got.at[k - 1], line_send.at[k - 1], line_recv.at[k - 1], line_at(k))
    for k in range(1, lines):
        line_copies[k].wait_recv()
        summed += line_got[k - 1].astype(F32)
    total[chip] = summed.astype(BF16)
    for group in (pair_copies, owner_copies, line_copies):
        started += list(group.values())

    pairs = tiles * (tiles + 1) // 2
    across, spread = [], []
    for g, (low, high) in enumerate(((0, pairs), (pairs, pairs + tiles * tiles // 2))):
        across.append([])
        spread_g = []
        for k in range(1, lines):
            piece = total.at[chip, :, low:high]
            spread_g.append(copy(piece, piece, spread_send.at[g, k - 1], spread_recv.at[g, k - 1], line_at(k)))
        piece = total.at[chip, :, low:high]
        across[g].append(copy(piece, piece, across_send.at[g, 0], across_recv.at[g, 0], pair))
        started += spread_g
        spread.append(spread_g)
    for g, (low, high) in enumerate(((0, pairs), (pairs, pairs + tiles * tiles // 2))):
        for k in range(1, lines):
            spread[g][k - 1].wait_recv()
            origin = lax.rem(line - k + lines, lines) * 2 + side
            piece = total.at[origin, :, low:high]
            across[g].append(copy(piece, piece, across_send.at[g, k], across_recv.at[g, k], pair))
        started += across[g]
    for c in across[0]:
        c.wait_recv()

    at_row = lax.broadcasted_iota(jnp.int32, (width, width), 0)
    at_column = lax.broadcasted_iota(jnp.int32, (width, width), 1)
    eye = (at_row == at_column).astype(F32)
    inverse_copies = []
    for s in range(slots):
        at = 0
        for i in range(tiles):
            for j in range(i, tiles):
                tile = tile_of(s, at)
                full[TILE * i:TILE * (i + 1), TILE * j:TILE * (j + 1)] = tile
                if j > i:
                    full[TILE * j:TILE * (j + 1), TILE * i:TILE * (i + 1)] = tile.T
                at += 1
        factor = full[...]
        damped = factor + (jnp.sum(factor * eye) * (0.05 / width)) * eye
        scale = lax.rsqrt(jnp.sum(damped * damped) + 1e-06)
        near = damped * scale
        approx = 2.0 * eye - near
        near_low = near.astype(BF16)
        near = 2.0 * near - mm(near_low, near_low)
        for step in range(3):
            near_low = near.astype(BF16)
            approx = 2.0 * approx - mm(approx.astype(BF16), near_low)
            if step < 2:
                near = 2.0 * near - mm(near_low, near_low)
        inverse[core, s] = (approx * scale).astype(BF16)
        inverse_copies.append(copy(inverse.at[core, s], inverse.at[core, s], last_send.at[1, s], last_recv.at[1, s], partner))
    for c in across[1]:
        c.wait_recv()
    half_copies = []
    for s in range(slots):
        at = tiles * (tiles + 1) // 2
        for i in range(tiles // 2):
            for j in range(tiles):
                halves[core, s, TILE * i:TILE * (i + 1), TILE * j:TILE * (j + 1)] = tile_of(s, at).astype(BF16)
                at += 1
        half_copies.append(copy(halves.at[core, s], halves.at[core, s], last_send.at[0, s], last_recv.at[0, s], partner))
    started += half_copies + inverse_copies
    for s in range(slots):
        half_copies[s].wait_recv()
        inverse_copies[s].wait_recv()
        grad = halves[:, s].reshape(width, width)
        left = mm(inverse[0, s], grad)
        out[s] = mm(left.astype(BF16), inverse[1, s]).astype(BF16)
    for c in started:
        c.wait_send()


def solution(mesh):
    owners = mesh.shape["owner"]
    chips = mesh.shape["dp"] // 2

    def local(edge_in, edge_grad, row_mask, layer_at):
        layers, rows, width = edge_in.shape
        slots = layers // owners
        rows_all = rows * mesh.shape["dp"] * owners
        tiles = width // TILE
        count = tiles * (tiles + 1) // 2 + tiles * tiles // 2
        part = TILE // chips
        lines = chips // 2
        others = max(owners - 1, 1)
        vmem = pl.BlockSpec(memory_space=pltpu.VMEM)
        dma = pltpu.SemaphoreType.DMA
        return pl.pallas_call(
            functools.partial(kernel, owners, chips, slots, rows, width, rows_all),
            out_shape=jax.ShapeDtypeStruct((slots, width, width), BF16),
            in_specs=[vmem, vmem, vmem, pl.BlockSpec(memory_space=pltpu.SMEM)],
            out_specs=vmem,
            scratch_shapes=[
                pltpu.VMEM((owners, slots, chips, count, part, TILE), BF16),
                pltpu.VMEM((owners, slots, chips, count, part, TILE), BF16),
                pltpu.VMEM((owners, slots, chips, count, part, TILE), BF16),
                pltpu.VMEM((owners, lines, slots, count, part, TILE), BF16),
                pltpu.VMEM((others, lines, slots, count, part, TILE), BF16),
                pltpu.VMEM((others, lines, slots, count, part, TILE), BF16),
                pltpu.VMEM((lines - 1, slots, count, part, TILE), BF16),
                pltpu.VMEM((lines - 1, slots, count, part, TILE), BF16),
                pltpu.VMEM((chips, slots, count, part, TILE), BF16),
                pltpu.VMEM((width, width), F32),
                pltpu.VMEM((2, slots, width // 2, width), BF16),
                pltpu.VMEM((2, slots, width, width), BF16),
                dma((owners, slots)), dma((owners, slots)),
                dma((owners, lines)), dma((owners, lines)),
                dma((others, lines)), dma((others, lines)),
                dma((lines - 1,)), dma((lines - 1,)),
                dma((2, slots)), dma((2, slots)),
                dma((2, lines - 1)), dma((2, lines - 1)),
                dma((2, lines)), dma((2, lines)),
            ],
            compiler_params=pltpu.CompilerParams(
                collective_id=0, has_side_effects=True, vmem_limit_bytes=60 * 1024 * 1024,
            ),
        )(edge_in, edge_grad, row_mask, layer_at)

    in_specs = (
        P(None, ("dp", "owner"), None),
        P(None, ("dp", "owner"), None),
        P(None, ("dp", "owner")),
        P(),
    )
    return jax.shard_map(local, mesh=mesh, in_specs=in_specs, out_specs=P("owner", None, None), check_vma=False)
```

```python
import functools
import math

import jax
import jax.numpy as jnp
from jax import lax
from jax.experimental import pallas as pl
from jax.experimental.pallas import tpu as pltpu
from jax.sharding import PartitionSpec as P

MESH = pl.DeviceIdType.MESH
F32 = jnp.float32
BF16 = jnp.bfloat16
TILE = 128


def mm(left, right):
    return jnp.dot(left, right, preferred_element_type=F32)


def mm_rows(left, right):
    return lax.dot_general(left, right, (((0,), (0,)), ((), ())), preferred_element_type=F32)


def kernel(
    owners, chips, slots, rows, width, rows_all,
    edge_in, edge_grad, mask, layer_at, out,
    give, got, split, pair_got, crossing, owner_got, passing, line_got, total, full, halves, inverse,
    core_send, core_recv, pair_send, pair_recv, owner_send, owner_recv,
    line_send, line_recv, last_send, last_recv,
    spread_send, spread_recv, across_send, across_recv,
):
    dp = lax.axis_index("dp")
    me = lax.axis_index("owner")
    chip = dp // 2
    core = lax.rem(dp, 2)
    other = 1 - core
    half = width // 2
    part = TILE // chips
    tiles = width // TILE
    lines = chips // 2
    line = chip // 2
    side = lax.rem(chip, 2)

    barrier = pltpu.get_barrier_semaphore()

    def owner_at(k):
        return {"dp": dp, "owner": lax.rem(me + k, owners)}

    def line_at(k):
        return {"dp": (lax.rem(line + k, lines) * 2 + side) * 2 + core, "owner": me}

    pair = {"dp": (line * 2 + 1 - side) * 2 + core, "owner": me}

    partner = {"dp": chip * 2 + other, "owner": me}
    peers = [owner_at(k) for k in range(1, owners)]
    peers += [line_at(k) for k in range(1, lines)]
    peers += [pair, partner]
    for peer in peers:
        pl.semaphore_signal(barrier, inc=1, device_id=peer, device_id_type=MESH)

    def copy(src, dst, send, recv, device):
        made = pltpu.make_async_remote_copy(
            src_ref=src, dst_ref=dst, send_sem=send, recv_sem=recv,
            device_id=device, device_id_type=MESH,
        )
        made.start()
        return made

    started = []

    def terms(c, q, s):
        layer = layer_at[q * slots + s]
        inputs, grads = edge_in[layer], edge_grad[layer]
        column = jnp.broadcast_to(mask[pl.ds(layer, 1), :].astype(F32), (TILE, rows)).T
        column = jnp.concatenate([column] * tiles, axis=1)
        first = c == 0
        values = (jnp.where(first, inputs, grads).astype(F32) * column).astype(BF16)
        left = jnp.where(first, inputs[:, :half], inputs[:, half:])
        made = [mm_rows(values[:, TILE * i:TILE * (i + 1)], values[:, TILE * i:]) for i in range(tiles)]
        made.append(mm_rows(left, grads))
        return made

    def pack(ref, sums):
        at = 0
        for i in range(tiles):
            strip = sums[i] * (1.0 / rows_all)
            for j in range(tiles - i):
                tile = strip[:, TILE * j:TILE * (j + 1)].reshape(chips, part, TILE)
                ref[:, at] = tile.astype(BF16)
                at += 1
        cross = sums[tiles] * (1.0 / math.sqrt(rows_all))
        for i in range(tiles // 2):
            for j in range(tiles):
                tile = cross[TILE * i:TILE * (i + 1), TILE * j:TILE * (j + 1)].reshape(chips, part, TILE)
                ref[:, at] = tile.astype(BF16)
                at += 1

    def tile_of(s, at):
        return total[:, s, at].astype(F32).reshape(TILE, TILE)

    order = list(range(1, lines)) + [0]
    early, middle = order[:2], order[2:-1]
    late = [(0, order[0])] + [(o, k) for k in middle for o in range(1, owners)]
    late += [(0, k) for k in order[1:-1]] + [(o, 0) for o in range(1, owners)] + [(0, 0)]
    pair_copies = {}

    def send_pair(o, k):
        far = lax.rem(line + k, lines) * 2 + 1 - side
        pair_copies[o, k] = copy(split.at[o, :, far], pair_got.at[o, k], pair_send.at[o, k], pair_recv.at[o, k], pair)

    for o in list(range(1, owners)) + [0]:
        q = lax.rem(me + o, owners)
        core_copies = []
        for s in range(slots):
            pack(give.at[o, s], terms(other, q, s))
            if not started and not core_copies:
                pl.semaphore_wait(barrier, len(peers))
            core_copies.append(copy(give.at[o, s], got.at[o, s], core_send.at[o, s], core_recv.at[o, s], partner))
        for s in range(slots):
            pack(split.at[o, s], terms(core, q, s))
            core_copies[s].wait_recv()
            split[o, s] = (split[o, s].astype(F32) + got[o, s].astype(F32)).astype(BF16)
        started += core_copies
        for k in early if o else ():
            send_pair(o, k)
    for o, k in late:
        send_pair(o, k)

    owner_copies, line_copies = {}, {}
    for o, k in [(o, k) for o in range(1, owners) for k in early] + late:
        near = lax.rem(line + k, lines) * 2 + side
        pair_copies[o, k].wait_recv()
        summed = split[o, :, near].astype(F32) + pair_got[o, k].astype(F32)
        if o:
            crossing[o - 1, k] = summed.astype(BF16)
            owner_copies[o, k] = copy(crossing.at[o - 1, k], owner_got.at[o - 1, k], owner_send.at[o - 1, k], owner_recv.at[o - 1, k], owner_at(o))
            continue
        for p in range(1, owners):
            owner_copies[p, k].wait_recv()
            summed += owner_got[p - 1, k].astype(F32)
        if k:
            passing[k - 1] = summed.astype(BF16)
            line_copies[k] = copy(passing.at[k - 1], line_got.at[k - 1], line_send.at[k - 1], line_recv.at[k - 1], line_at(k))
    for k in range(1, lines):
        line_copies[k].wait_recv()
        summed += line_got[k - 1].astype(F32)
    total[chip] = summed.astype(BF16)
    for group in (pair_copies, owner_copies, line_copies):
        started += list(group.values())

    pairs = tiles * (tiles + 1) // 2
    across, spread = [], []
    for g, (low, high) in enumerate(((0, pairs), (pairs, pairs + tiles * tiles // 2))):
        across.append([])
        spread_g = []
        for k in range(1, lines):
            piece = total.at[chip, :, low:high]
            spread_g.append(copy(piece, piece, spread_send.at[g, k - 1], spread_recv.at[g, k - 1], line_at(k)))
        piece = total.at[chip, :, low:high]
        across[g].append(copy(piece, piece, across_send.at[g, 0], across_recv.at[g, 0], pair))
        started += spread_g
        spread.append(spread_g)
    for g, (low, high) in enumerate(((0, pairs), (pairs, pairs + tiles * tiles // 2))):
        for k in range(1, lines):
            spread[g][k - 1].wait_recv()
            origin = lax.rem(line - k + lines, lines) * 2 + side
            piece = total.at[origin, :, low:high]
            across[g].append(copy(piece, piece, across_send.at[g, k], across_recv.at[g, k], pair))
        started += across[g]
    for c in across[0]:
        c.wait_recv()

    at_row = lax.broadcasted_iota(jnp.int32, (width, width), 0)
    at_column = lax.broadcasted_iota(jnp.int32, (width, width), 1)
    eye = (at_row == at_column).astype(F32)
    inverse_copies = []
    for s in range(slots):
        at = 0
        for i in range(tiles):
            for j in range(i, tiles):
                tile = tile_of(s, at)
                full[TILE * i:TILE * (i + 1), TILE * j:TILE * (j + 1)] = tile
                if j > i:
                    full[TILE * j:TILE * (j + 1), TILE * i:TILE * (i + 1)] = tile.T
                at += 1
        factor = full[...]
        damped = factor + (jnp.sum(factor * eye) * (0.05 / width)) * eye
        scale = lax.rsqrt(jnp.sum(damped * damped) + 1e-06)
        near = damped * scale
        approx = 2.0 * eye - near
        near_low = near.astype(BF16)
        near = 2.0 * near - mm(near_low, near_low)
        for step in range(3):
            near_low = near.astype(BF16)
            approx = 2.0 * approx - mm(approx.astype(BF16), near_low)
            if step < 2:
                near = 2.0 * near - mm(near_low, near_low)
        inverse[core, s] = (approx * scale).astype(BF16)
        inverse_copies.append(copy(inverse.at[core, s], inverse.at[core, s], last_send.at[1, s], last_recv.at[1, s], partner))
    for c in across[1]:
        c.wait_recv()
    half_copies = []
    for s in range(slots):
        at = tiles * (tiles + 1) // 2
        for i in range(tiles // 2):
            for j in range(tiles):
                halves[core, s, TILE * i:TILE * (i + 1), TILE * j:TILE * (j + 1)] = tile_of(s, at).astype(BF16)
                at += 1
        half_copies.append(copy(halves.at[core, s], halves.at[core, s], last_send.at[0, s], last_recv.at[0, s], partner))
    started += half_copies + inverse_copies
    for s in range(slots):
        half_copies[s].wait_recv()
        inverse_copies[s].wait_recv()
        grad = halves[:, s].reshape(width, width)
        left = mm(inverse[0, s], grad)
        out[s] = mm(left.astype(BF16), inverse[1, s]).astype(BF16)
    for c in started:
        c.wait_send()


def solution(mesh):
    owners = mesh.shape["owner"]
    chips = mesh.shape["dp"] // 2

    def local(edge_in, edge_grad, row_mask, layer_at):
        layers, rows, width = edge_in.shape
        slots = layers // owners
        rows_all = rows * mesh.shape["dp"] * owners
        tiles = width // TILE
        count = tiles * (tiles + 1) // 2 + tiles * tiles // 2
        part = TILE // chips
        lines = chips // 2
        others = max(owners - 1, 1)
        vmem = pl.BlockSpec(memory_space=pltpu.VMEM)
        dma = pltpu.SemaphoreType.DMA
        return pl.pallas_call(
            functools.partial(kernel, owners, chips, slots, rows, width, rows_all),
            out_shape=jax.ShapeDtypeStruct((slots, width, width), BF16),
            in_specs=[vmem, vmem, vmem, pl.BlockSpec(memory_space=pltpu.SMEM)],
            out_specs=vmem,
            scratch_shapes=[
                pltpu.VMEM((owners, slots, chips, count, part, TILE), BF16),
                pltpu.VMEM((owners, slots, chips, count, part, TILE), BF16),
                pltpu.VMEM((owners, slots, chips, count, part, TILE), BF16),
                pltpu.VMEM((owners, lines, slots, count, part, TILE), BF16),
                pltpu.VMEM((others, lines, slots, count, part, TILE), BF16),
                pltpu.VMEM((others, lines, slots, count, part, TILE), BF16),
                pltpu.VMEM((lines - 1, slots, count, part, TILE), BF16),
                pltpu.VMEM((lines - 1, slots, count, part, TILE), BF16),
                pltpu.VMEM((chips, slots, count, part, TILE), BF16),
                pltpu.VMEM((width, width), F32),
                pltpu.VMEM((2, slots, width // 2, width), BF16),
                pltpu.VMEM((2, slots, width, width), BF16),
                dma((owners, slots)), dma((owners, slots)),
                dma((owners, lines)), dma((owners, lines)),
                dma((others, lines)), dma((others, lines)),
                dma((lines - 1,)), dma((lines - 1,)),
                dma((2, slots)), dma((2, slots)),
                dma((2, lines - 1)), dma((2, lines - 1)),
                dma((2, lines)), dma((2, lines)),
            ],
            compiler_params=pltpu.CompilerParams(
                collective_id=0, has_side_effects=True, vmem_limit_bytes=60 * 1024 * 1024,
            ),
        )(edge_in, edge_grad, row_mask, layer_at)

    in_specs = (
        P(None, ("dp", "owner"), None),
        P(None, ("dp", "owner"), None),
        P(None, ("dp", "owner")),
        P(),
    )
    return jax.shard_map(local, mesh=mesh, in_specs=in_specs, out_specs=P("owner", None, None), check_vma=False)
```
